32 devices in a mesh: rep: 2 (over x), gx: 16 (over z, y, core).
Axes of the slice: x: 2, y: 2, z: 4, core: 2. Of those that a mesh axis runs over, the one named last changes fastest.
Arguments:
- positions: float32 [3, 131072], P(None, ('rep', 'gx')), parts along dimension 1, may hold values from 0 to 128, as said below
- polar: float32 [131072], P(('rep', 'gx')), parts along dimension 0, may hold values from 0.25 to 1
- field_ext: float32 [3, 131072], P(None, ('rep', 'gx')), parts along dimension 1, may hold values from -10 to 10
- tile_atom: int32 [131072], P(('rep', 'gx')), parts along dimension 0, may hold values from 0 to 4095, as said below
- tile_list: int32 [1024, 3], P(('rep', 'gx')), parts along dimension 0, may hold values from 0 to 63, as said below
- image_shift: int32 [2, 1024, 3], P(None, ('rep', 'gx')), parts along dimension 1, may hold values from 0 to 1, as said below
Outputs:
- dipoles: float32 [3, 131072], P(None, ('rep', 'gx')), parts along dimension 1
- residual: float32 [3, 131072], P(None, ('rep', 'gx')), parts along dimension 1
The draws below stay inside these ranges and needn't reach their ends.
There are 2 independent parts, one for each index of `rep`. The reference program is written for one: setup_inputs(seed, part) draws one part's arguments, and reference() takes and returns one part's arrays. A program takes and returns all parts, laid end to end along the dimension named above; each array names one. Nothing has to cross between parts.
Inputs may be any that keep to these rules, and one draw needn't show every extreme that they name: `positions`: coordinates lie in a box of 64 by 128 by 64; the atoms of slab s have first coordinate between 4 s and 4 s + 4; no two atoms, and no atom and a periodic image of another, are closer than 1.4. `tile_atom`: for each slab, a permutation of 0 to 4095. `tile_list`: entry 0 of a tile is the tile's own index within its slab. Entry n of a tile of slab s names tile n of slab s if n < 32, else tile n - 32 of slab s + 1 (slab 0 after the last). `image_shift`: offsets along the second and third coordinates in box lengths, one pair for each entry of tile_list; zero for entry 0.
All inputs are finite; a program needn't handle non-finite values.
Results may differ from the reference program's by a relative error of at most 0.0003.
Values sent between devices are 32-bit elements; how exact they have to be, the bound alone decides.
A program may use at most 64 MiB of HBM per device.

```python
import math
import jax
import jax.numpy as jnp
from jax import lax

TILE = 128
TILES_DEV = 32
NB = 3
ITERS = 4
TILES = 512
ATOMS_DEV = 4096
ATOMS = 65536


def atom_order(key):
    slab_count = ATOMS // ATOMS_DEV
    keys = jax.random.split(jax.random.fold_in(key, 11), slab_count)

    def one_slab(slab_key):
        return jax.random.permutation(slab_key, ATOMS_DEV).astype(jnp.int32)
    return jax.vmap(one_slab)(keys).reshape(ATOMS)


def lattice_places():
    slot_ids = jnp.arange(ATOMS, dtype=jnp.int32)
    slab_ids = slot_ids // ATOMS_DEV
    local_ids = slot_ids % ATOMS_DEV
    tile_ids = local_ids // TILE
    within = local_ids % TILE
    rows_z = TILES_DEV // 8
    cell_y = tile_ids // rows_z
    cell_z = tile_ids % rows_z
    layer_id = within // 64
    along_y = within // 8 % 8
    along_z = within % 8
    coord_x = 4 * slab_ids + 2 * layer_id + 1
    coord_y = 2 * (8 * cell_y + along_y) + 1
    coord_z = 2 * (8 * cell_z + along_z) + 1
    return (jnp.stack([coord_x, coord_y, coord_z]).astype(jnp.float32), slab_ids)


def draw_tile_atom(key, part):
    return atom_order(key)


def draw_positions(key, part):
    order_ids = atom_order(key)
    base, slab_ids = lattice_places()
    jitter_key = jax.random.fold_in(key, 23)
    jitter = jax.random.uniform(jitter_key, (3, ATOMS), jnp.float32, -0.3, 0.3)
    placed = base + jitter
    target = slab_ids * ATOMS_DEV + order_ids
    return jnp.zeros((3, ATOMS), jnp.float32).at[:, target].set(placed)


def draw_field_ext(key, part):
    slab_count = ATOMS // ATOMS_DEV
    slab_ids = jnp.arange(ATOMS, dtype=jnp.int32) // ATOMS_DEV
    ramp = slab_ids.astype(jnp.float32) / (slab_count - 1)
    noise = jnp.clip(jax.random.normal(key, (3, ATOMS), jnp.float32), -5.0, 5.0)
    return noise * (0.6 + 1.2 * ramp)


def neighbour_entries(key):
    score_key = jax.random.fold_in(key, 37)
    scores = jax.random.randint(score_key, (TILES, 7), 0, 1 << 20) * 8 + jnp.arange(7, dtype=jnp.int32)[None, :]
    picked = jnp.argsort(scores, axis=1)[:, :NB - 1].astype(jnp.int32) + 1
    step_x = picked // 4
    step_y = picked // 2 % 2
    step_z = picked % 2
    rows_z = TILES_DEV // 8
    tile_ids = jnp.arange(TILES, dtype=jnp.int32) % TILES_DEV
    cell_y = (tile_ids // rows_z)[:, None]
    cell_z = (tile_ids % rows_z)[:, None]
    next_y = cell_y + step_y
    next_z = cell_z + step_z
    image_y = next_y // 8
    image_z = next_z // rows_z
    named = step_x * TILES_DEV + next_y % 8 * rows_z + next_z % rows_z
    lists = jnp.concatenate([tile_ids[:, None], named], axis=1).astype(jnp.int32)
    zeros_col = jnp.zeros((TILES, 1), jnp.int32)
    shifts = jnp.stack([jnp.concatenate([zeros_col, image_y], axis=1), jnp.concatenate([zeros_col, image_z], axis=1)]).astype(jnp.int32)
    return (lists, shifts)


def draw_tile_list(key, part):
    lists, shifts = neighbour_entries(key)
    return lists


def draw_image_shift(key, part):
    lists, shifts = neighbour_entries(key)
    return shifts


def shard_levels(own_key, shape, cuts, least, largest):
    factor_of = 1.0
    for position, blocks in cuts:
        steps = jax.random.uniform(jax.random.fold_in(jax.random.fold_in(own_key, 6), position), (blocks,), jnp.float32, least / len(cuts), largest / len(cuts))
        factor_of = factor_of * jnp.repeat(jnp.exp(steps), shape[position] // blocks).reshape((-1,) + (1,) * (len(shape) - 1 - position))
    return factor_of


def setup_inputs(seed: int = 0, part: int = 0) -> dict:
    splits = jax.random.split(jax.random.key(seed), 7)
    part_splits = jax.random.split(jax.random.fold_in(splits[6], part), 7)
    positions = draw_positions(jax.random.fold_in(jax.random.fold_in(splits[6], part), 71), part)
    polar = jnp.clip(jnp.exp(math.log(1.0) - 1.3862944 * jax.random.uniform(part_splits[1], (ATOMS,), jnp.float32) ** shard_levels(part_splits[1], (ATOMS,), ((0, 16),), -0.2, 0.2)), 0.25, 1.0)
    field_ext = draw_field_ext(jax.random.fold_in(jax.random.fold_in(splits[6], part), 71), part)
    tile_atom = draw_tile_atom(jax.random.fold_in(jax.random.fold_in(splits[6], part), 71), part)
    tile_list = draw_tile_list(jax.random.fold_in(jax.random.fold_in(splits[6], part), 71), part)
    image_shift = draw_image_shift(jax.random.fold_in(jax.random.fold_in(splits[6], part), 71), part)
    return {"positions": positions, "polar": polar, "field_ext": field_ext, "tile_atom": tile_atom, "tile_list": tile_list, "image_shift": image_shift}


thole_factor = 0.39

def pair_block(place_left, root_left, moment_left, place_right, root_right, moment_right, weights, self_flags):
    offset_x = place_right[:, 0, None, :] - place_left[:, 0, :, None]
    offset_y = place_right[:, 1, None, :] - place_left[:, 1, :, None]
    offset_z = place_right[:, 2, None, :] - place_left[:, 2, :, None]
    dist_sq = offset_x * offset_x + offset_y * offset_y + offset_z * offset_z
    tile_width = place_left.shape[2]
    row_ids = lax.broadcasted_iota(jnp.int32, (tile_width, tile_width), 0)
    column_ids = lax.broadcasted_iota(jnp.int32, (tile_width, tile_width), 1)
    same_atom = jnp.logical_and(self_flags[:, None, None] > 0, (row_ids == column_ids)[None])
    dist_sq = jnp.where(same_atom, 1.0, dist_sq)
    inv_dist = lax.rsqrt(dist_sq)
    distance = dist_sq * inv_dist
    damp_arg = thole_factor * dist_sq * distance / (root_left[:, :, None] * root_right[:, None, :])
    decay = jnp.exp(-damp_arg)
    inv_cube = jnp.where(same_atom, 0.0, weights[:, None, None] * inv_dist * inv_dist * inv_dist)
    coeff_three = (1.0 - decay) * inv_cube
    coeff_five = 3.0 * (1.0 - (1.0 + damp_arg) * decay) * inv_cube * inv_dist * inv_dist
    offsets = (offset_x, offset_y, offset_z)
    proj_right = offset_x * moment_right[:, 0, None, :] + offset_y * moment_right[:, 1, None, :] + offset_z * moment_right[:, 2, None, :]
    proj_left = offset_x * moment_left[:, 0, :, None] + offset_y * moment_left[:, 1, :, None] + offset_z * moment_left[:, 2, :, None]
    lift_right = coeff_five * proj_right
    lift_left = coeff_five * proj_left
    field_left = jnp.stack([lax.optimization_barrier(jnp.sum(lift_right * offsets[component] - coeff_three * moment_right[:, component, None, :], axis=2)) for component in range(3)], axis=1)
    field_right = jnp.stack([lax.optimization_barrier(jnp.sum(lift_left * offsets[component] - coeff_three * moment_left[:, component, :, None], axis=1)) for component in range(3)], axis=1)
    return (field_left, field_right)

def slab_fields(window_place, window_root, window_moment, left_index, right_index, image_vec, weights, self_flags):
    entries = left_index.shape[0]
    block_size = math.gcd(entries, 32)
    window_size = window_place.shape[0]
    tile_width = window_place.shape[2]
    slot_ids = jnp.arange(window_size, dtype=jnp.int32)

    def accumulate(summed, first_entry):
        left_rows = lax.dynamic_slice_in_dim(left_index, first_entry, block_size)
        right_rows = lax.dynamic_slice_in_dim(right_index, first_entry, block_size)
        image_rows = lax.dynamic_slice_in_dim(image_vec, first_entry, block_size)
        weight_rows = lax.dynamic_slice_in_dim(weights, first_entry, block_size)
        flag_rows = lax.dynamic_slice_in_dim(self_flags, first_entry, block_size)
        place_left = jnp.take(window_place, left_rows, axis=0)
        place_right = jnp.take(window_place, right_rows, axis=0) + image_rows[:, :, None]
        field_left, field_right = pair_block(place_left, jnp.take(window_root, left_rows, axis=0), jnp.take(window_moment, left_rows, axis=0), place_right, jnp.take(window_root, right_rows, axis=0), jnp.take(window_moment, right_rows, axis=0), weight_rows, flag_rows)
        hit_left = (left_rows[:, None] == slot_ids[None, :]).astype(jnp.float32)
        hit_right = (right_rows[:, None] == slot_ids[None, :]).astype(jnp.float32)
        summed = summed + jnp.einsum('ew,ef->wf', hit_left, field_left.reshape(block_size, 3 * tile_width), precision=lax.Precision.HIGHEST)
        summed = summed + jnp.einsum('ew,ef->wf', hit_right, field_right.reshape(block_size, 3 * tile_width), precision=lax.Precision.HIGHEST)
        return (summed, None)
    first_entries = jnp.arange(0, entries, block_size, dtype=jnp.int32)
    summed, _ = lax.scan(accumulate, jnp.zeros((window_size, 3 * tile_width), jnp.float32), first_entries)
    return summed.reshape(window_size, 3, tile_width)

def image_vectors(lists, shifts, last_flag, tile_count, box_x, box_y, box_z):
    crossing = lists >= tile_count
    wrapped = jnp.where(jnp.logical_and(crossing, last_flag), box_x, 0.0)
    vectors = jnp.stack([wrapped, shifts[0].astype(jnp.float32) * box_y, shifts[1].astype(jnp.float32) * box_z], axis=-1)
    return vectors.reshape(-1, 3)

def reference(positions, polar, field_ext, tile_atom, tile_list, image_shift):
    slab_count = TILES // TILES_DEV
    slot_atom = jnp.arange(ATOMS, dtype=jnp.int32) // ATOMS_DEV * ATOMS_DEV + tile_atom
    tiled_place = positions[:, slot_atom].reshape(3, TILES, TILE).transpose(1, 0, 2)
    tiled_polar = polar[slot_atom].reshape(TILES, TILE)
    tiled_root = jnp.sqrt(tiled_polar)
    tiled_rhs = field_ext[:, slot_atom].reshape(3, TILES, TILE).transpose(1, 0, 2)
    box_x = 4.0 * slab_count
    box_y = 128.0
    box_z = 2.0 * TILES_DEV
    last_flag = (jnp.arange(TILES, dtype=jnp.int32) // TILES_DEV == slab_count - 1)[:, None]
    image_all = image_vectors(tile_list, image_shift, last_flag, TILES_DEV, box_x, box_y, box_z)
    entry_ids = jnp.arange(NB, dtype=jnp.int32)
    own_left = jnp.repeat(jnp.arange(TILES_DEV, dtype=jnp.int32), NB)
    own_weights = jnp.tile(jnp.where(entry_ids == 0, 0.5, 1.0), TILES_DEV)
    own_self = jnp.tile((entry_ids == 0).astype(jnp.int32), TILES_DEV)
    slab_ids = jnp.arange(slab_count, dtype=jnp.int32)

    def apply_operator(moment):

        def per_slab(summed, slab):
            first = slab * TILES_DEV
            after = (slab + 1) % slab_count * TILES_DEV
            window_place = jnp.concatenate([lax.dynamic_slice_in_dim(tiled_place, first, TILES_DEV), lax.dynamic_slice_in_dim(tiled_place, after, TILES_DEV)], axis=0)
            window_root = jnp.concatenate([lax.dynamic_slice_in_dim(tiled_root, first, TILES_DEV), lax.dynamic_slice_in_dim(tiled_root, after, TILES_DEV)], axis=0)
            window_moment = jnp.concatenate([lax.dynamic_slice_in_dim(moment, first, TILES_DEV), lax.dynamic_slice_in_dim(moment, after, TILES_DEV)], axis=0)
            lists = lax.dynamic_slice_in_dim(tile_list, first, TILES_DEV).reshape(-1)
            images = lax.dynamic_slice_in_dim(image_all, first * NB, TILES_DEV * NB)
            window = slab_fields(window_place, window_root, window_moment, own_left, lists, images, own_weights, own_self)
            summed = lax.dynamic_update_slice_in_dim(summed, lax.dynamic_slice_in_dim(summed, first, TILES_DEV) + window[:TILES_DEV], first, 0)
            summed = lax.dynamic_update_slice_in_dim(summed, lax.dynamic_slice_in_dim(summed, after, TILES_DEV) + window[TILES_DEV:], after, 0)
            return (summed, None)
        fields, _ = lax.scan(per_slab, jnp.zeros((TILES, 3, TILE), jnp.float32), slab_ids)
        return moment / tiled_polar[:, None, :] - fields
    solution = jnp.zeros_like(tiled_rhs)
    resid = tiled_rhs
    direction = tiled_rhs
    norm_now = jnp.sum(resid * resid)
    for iteration in range(ITERS):
        applied = apply_operator(direction)
        step_size = norm_now / jnp.sum(direction * applied)
        solution = solution + step_size * direction
        resid = resid - step_size * applied
        norm_next = jnp.sum(resid * resid)
        direction = resid + norm_next / norm_now * direction
        norm_now = norm_next
    dipoles = jnp.zeros((3, ATOMS), jnp.float32).at[:, slot_atom].set(solution.transpose(1, 0, 2).reshape(3, ATOMS))
    residual = jnp.zeros((3, ATOMS), jnp.float32).at[:, slot_atom].set(resid.transpose(1, 0, 2).reshape(3, ATOMS))
    return (dipoles, residual)
```

```python
import functools

import jax
import jax.numpy as jnp
from jax import lax
from jax.experimental import pallas as pl
from jax.experimental.pallas import tpu as pltpu
from jax.sharding import PartitionSpec as P

ITERS = 4
MESH = pl.DeviceIdType.MESH
thole_factor = 0.39
ROWS = 16
F32 = jnp.float32
BF16 = jnp.bfloat16


def split_two(value):
    high = value.astype(BF16)
    return high, (value - high.astype(F32)).astype(BF16)


def split_three(value):
    high = value.astype(BF16)
    rest = value - high.astype(F32)
    middle = rest.astype(BF16)
    return high, middle, (rest - middle.astype(F32)).astype(BF16)


def gather_tile(row, source, tiles):
    width = 128
    inner = jnp.broadcast_to(row & (width - 1), (8, width))
    outer = jnp.broadcast_to(row >> 7, (8, width))
    value = jnp.zeros((8, width), F32)
    for tile in range(tiles):
        picked = jnp.take_along_axis(
            source[pl.ds(tile * 8, 8), :], inner, axis=1, mode="promise_in_bounds"
        )
        value = jnp.where(outer == tile, picked, value)
    return value


def tiling_kernel(
    tiles,
    links,
    list_ref,
    shift_ref,
    place_ref,
    polar_ref,
    field_ref,
    atom_ref,
    out_ref,
    inverse,
    hits,
    image,
    feat,
):
    width = 128
    near = links - 1
    for tile in range(tiles):
        lanes = pl.ds(tile * width, width)
        feat[tile * 8 : tile * 8 + 3, :] = place_ref[:, lanes]
        feat[tile * 8 + 3 : tile * 8 + 6, :] = field_ref[:, lanes]
        feat[tile * 8 + 6 : tile * 8 + 7, :] = polar_ref[:, lanes]
        feat[tile * 8 + 7 : tile * 8 + 8, :] = jnp.ones((1, width), F32)
    sub_ids = lax.broadcasted_iota(jnp.int32, (8, width), 0)

    def fill(tile, carry):
        value = gather_tile(atom_ref[pl.ds(tile, 1), :], feat, tiles)
        root = lax.rsqrt(value)
        value = jnp.where(sub_ids == 7, pltpu.roll(root, 1, 0), value)
        out_ref[pl.ds(pl.multiple_of(tile * 8, 8), 8), :] = value
        return carry

    lax.fori_loop(0, tiles, fill, 0)

    lane_ids = lax.broadcasted_iota(jnp.int32, (width, width), 0)
    tile_ids = lax.broadcasted_iota(jnp.int32, (tiles, width), 0)
    lane_row = lax.broadcasted_iota(jnp.int32, (tiles, width), 1).astype(F32)

    def invert(tile, total):
        row = atom_ref[pl.ds(tile, 1), :]
        outer = tile_ids == (row >> 7)
        number = jnp.full((tiles, width), tile, jnp.int32).astype(F32)
        left = jnp.concatenate(
            [jnp.where(outer, number, 0.0), jnp.where(outer, lane_row, 0.0)], axis=0
        ).astype(BF16)
        right = jnp.where(lane_ids == (row & (width - 1)), 1.0, 0.0).astype(BF16)
        return total + lax.dot_general(
            left, right, (((1,), (1,)), ((), ())), preferred_element_type=F32
        )

    found = lax.fori_loop(0, tiles, invert, jnp.zeros((2 * tiles, width), F32))
    inverse[...] = (found[:tiles] * float(width) + found[tiles:]).astype(jnp.int32)

    lane_one = lax.broadcasted_iota(jnp.int32, (1, width), 1)

    def name(tile, carry):
        for entry in range(near):
            slot = entry * tiles + tile
            named = list_ref[tile * links + entry + 1]
            hit = jnp.where((lane_one == named) | (lane_one == named + 2 * tiles), 1.0, 0.0)
            hits[pl.ds(slot, 1), :] = hit
            hits[pl.ds(near * tiles + slot, 1), :] = hit
            ones = jnp.ones((1, width), F32)
            crossing = jnp.where(named >= tiles, 1.0, 0.0)
            step_y = shift_ref[tile * links + entry + 1].astype(F32)
            step_z = shift_ref[(tiles + tile) * links + entry + 1].astype(F32)
            image[0, pl.ds(slot, 1), :] = ones * crossing
            image[1, pl.ds(slot, 1), :] = ones * step_y
            image[2, pl.ds(slot, 1), :] = ones * step_z
        return carry

    lax.fori_loop(0, tiles, name, 0)


def untiling_kernel(tiles, tiled_ref, inverse, dip_ref, res_ref):
    width = 128

    def give(tile, carry):
        value = gather_tile(inverse[pl.ds(tile, 1), :], tiled_ref, tiles)
        lanes = pl.ds(pl.multiple_of(tile * width, width), width)
        dip_ref[:, lanes] = value[0:3]
        res_ref[:, lanes] = value[3:6]
        return carry

    lax.fori_loop(0, tiles, give, 0)


def kernel(
    count,
    tiles,
    links,
    tiled_ref,
    hits_ref,
    image_ref,
    out_ref,
    window,
    pair_own,
    pair_back,
    pair_left,
    three_t,
    five_t,
    there,
    local,
    local_far,
    shift_left,
    shift_right,
    moments,
    minus,
    results,
    sent_w,
    ahead_w,
    sent_f,
    back_f,
    dots,
    pack_sem,
    w_sem,
    f_sem,
    dot_sem,
):
    width = 128
    near = links - 1
    me = lax.axis_index("gx")
    after = lax.rem(me + 1, count)
    before = lax.rem(me + count - 1, count)

    barrier = pltpu.get_barrier_semaphore()

    def greet(step, carry):
        pl.semaphore_signal(
            barrier, inc=1, device_id={"gx": lax.rem(me + step, count)}, device_id_type=MESH
        )
        return carry

    lax.fori_loop(1, count, greet, 0)

    sub_ids = lax.broadcasted_iota(jnp.int32, (8, width), 0)

    window[0 : tiles * 8, :] = tiled_ref[...]
    pl.semaphore_wait(barrier, count - 1)
    pack_copy = pltpu.make_async_remote_copy(
        src_ref=tiled_ref,
        dst_ref=window.at[pl.ds(tiles * 8, tiles * 8)],
        send_sem=pack_sem.at[0],
        recv_sem=pack_sem.at[1],
        device_id={"gx": before},
        device_id_type=MESH,
    )
    pack_copy.start()

    row_ids = lax.broadcasted_iota(jnp.int32, (16, width), 0)
    column_ids = lax.broadcasted_iota(jnp.int32, (16, width), 1)

    def pair_rows(columns, other, first, same):
        rows = slice(first, first + 16)
        off_x = other[0:1, :] - columns[rows, 0:1]
        off_y = other[1:2, :] - columns[rows, 1:2]
        off_z = other[2:3, :] - columns[rows, 2:3]
        dist_sq = off_x * off_x + off_y * off_y + off_z * off_z
        if same:
            mask = row_ids + first == column_ids
            dist_sq = jnp.where(mask, 1.0, dist_sq)
        inv = lax.rsqrt(dist_sq)
        inv_sq = inv * inv
        damp = dist_sq * dist_sq * inv * (columns[rows, 7:8] * (thole_factor * other[7:8, :]))
        decay = jnp.exp(-damp)
        inv_cube = inv * inv_sq
        if same:
            inv_cube = jnp.where(mask, 0.0, inv_cube)
        less = 1.0 - decay
        three = less * inv_cube
        five = 3.0 * (less - damp * decay) * (inv_cube * inv_sq)
        return three, five

    def store_pair(target, index, first, three, five):
        rows = slice(first, first + 16)
        more = slice(width + first, width + first + 16)
        high, low = split_two(five)
        target[index, rows, 0:width] = high
        target[index, rows, width : 2 * width] = low
        high, low = split_two(three)
        target[index, more, 0:width] = high
        target[index, more, width : 2 * width] = low

    def own_pairs(tile, carry):
        here = window[pl.ds(pl.multiple_of(tile * 8, 8), 8), :]
        columns = here.T
        for first in range(0, width, 16):
            three, five = pair_rows(columns, here, first, True)
            store_pair(pair_own, tile, first, three, five)
        return carry

    lax.fori_loop(0, tiles, own_pairs, 0)

    pack_copy.wait_recv()

    slots = near * tiles
    hit_own = hits_ref[0:slots, :].astype(BF16)
    hit_rows = hits_ref[...].T[0 : 2 * tiles].astype(BF16)

    def picked(matrix, values):
        high, middle, low = split_three(jnp.concatenate(values, axis=1))
        found = jnp.dot(
            matrix, jnp.concatenate([high, middle], axis=0), preferred_element_type=F32
        ) + jnp.dot(
            matrix,
            jnp.concatenate([low, jnp.zeros_like(low)], axis=0),
            preferred_element_type=F32,
        )
        return [found[:, part * width : (part + 1) * width] for part in range(len(values))]

    def middle_of(value):
        return jnp.floor(jnp.mean(value, axis=1, keepdims=True) + 0.5)

    both = [window[pl.ds(row, 2 * tiles, stride=8), :] for row in (0, 1, 2, 7)]
    named = picked(hit_own, both)
    there[pl.ds(7, slots, stride=8), :] = named[3]
    lengths = (jnp.where(me == count - 1, 4.0 * count, 0.0), 128.0, 2.0 * tiles)
    for axis in range(3):
        here = both[axis][0:tiles]
        here_middle = middle_of(here)
        local[axis] = here - here_middle
        far_middle = middle_of(named[axis])
        local_far[axis] = named[axis] - far_middle
        vector = image_ref[axis] * lengths[axis]
        moved = named[axis] + vector
        there[pl.ds(axis, slots, stride=8), :] = moved
        for entry in range(near):
            part = slice(entry * tiles, (entry + 1) * tiles)
            shift_left[axis, part, :] = here - (far_middle[part] + vector[part])
            shift_right[axis, part, :] = moved[part] - here_middle

    def far_pairs(tile, carry):
        here_rows = pl.ds(pl.multiple_of(tile * 8, 8), 8)
        here = window[here_rows, :]
        columns = here.T
        for entry in range(near):
            slot = entry * tiles + tile
            other = there[pl.ds(pl.multiple_of(slot * 8, 8), 8), :]
            for first in range(0, width, 16):
                three, five = pair_rows(columns, other, first, False)
                store_pair(pair_back, slot, first, three, five)
                three_t[entry, first : first + 16, :] = three
                five_t[entry, first : first + 16, :] = five
            three = three_t[entry].T
            five = five_t[entry].T
            for first in range(0, width, 16):
                store_pair(
                    pair_left, slot, first, three[first : first + 16], five[first : first + 16]
                )
        return carry

    lax.fori_loop(0, tiles, far_pairs, 0)
    minus[...] = jnp.zeros_like(minus)

    def build(vec, base_ref, size):
        base = [base_ref[axis] for axis in range(3)]
        along = base[0] * vec[0] + base[1] * vec[1] + base[2] * vec[2]

        def put(ref, row, value):
            ref[pl.ds(row, size, stride=ROWS), :] = value

        for axis in range(3):
            put(moments, axis, base[axis] * along)
            put(minus, axis, -vec[axis])
            for other in range(3):
                put(moments, 4 + 4 * axis + other, base[other] * vec[axis])
            put(moments, 7 + 4 * axis, vec[axis])
        put(moments, 3, along)

    def block_of(tile):
        rows = pl.ds(pl.multiple_of(tile * ROWS, ROWS), ROWS)
        return jnp.concatenate(
            [
                jnp.concatenate(split_three(moments[rows, :]), axis=0),
                jnp.concatenate(split_three(minus[rows, :]), axis=0),
            ],
            axis=1,
        )

    def product(block, weights, slot):
        out = jnp.dot(block, weights, preferred_element_type=F32)
        out = out[:, :width] + out[:, width:]
        results[pl.ds(pl.multiple_of(slot * ROWS, ROWS), ROWS), :] = (
            out[0:ROWS] + out[ROWS : 2 * ROWS]
        ) + out[2 * ROWS : 3 * ROWS]

    def combined(kind, shifts):
        def get(row):
            return results[pl.ds(kind * tiles * ROWS + row, tiles, stride=ROWS), :]

        parts = []
        for row in range(4):
            total = get(row)
            for axis in range(3):
                total = total - shifts[axis] * get(4 + 4 * axis + row)
            parts.append(total)
        return [parts[axis] - shifts[axis] * parts[3] for axis in range(3)]

    def shifts_of(ref, entry):
        return [ref[axis, entry * tiles : (entry + 1) * tiles, :] for axis in range(3)]

    alpha_inv = 1.0 / window[pl.ds(6, tiles, stride=8), :]

    def copy_w(turn):
        return pltpu.make_async_remote_copy(
            src_ref=sent_w.at[turn],
            dst_ref=ahead_w.at[turn],
            send_sem=w_sem.at[0, turn],
            recv_sem=w_sem.at[1, turn],
            device_id={"gx": before},
            device_id_type=MESH,
        )

    def copy_f(turn):
        return pltpu.make_async_remote_copy(
            src_ref=sent_f.at[turn],
            dst_ref=back_f.at[turn],
            send_sem=f_sem.at[0, turn],
            recv_sem=f_sem.at[1, turn],
            device_id={"gx": after},
            device_id_type=MESH,
        )

    def back_step(group, carry):
        for offset in range(4):
            tile = group * 4 + offset
            block = block_of(tile)
            product(block, pair_own[tile], tile)
            for entry in range(near):
                slot = entry * tiles + tile
                product(block, pair_back[slot], tiles + slot)
        return carry

    def left_step(group, carry):
        for offset in range(4):
            tile = group * 4 + offset
            for entry in range(near):
                slot = entry * tiles + tile
                product(block_of(slot), pair_left[slot], tiles + slot)
        return carry

    def applied(turn, vec):
        build(vec, local, tiles)
        lax.fori_loop(0, tiles // 4, back_step, 0)
        back = [combined(1 + entry, shifts_of(shift_right, entry)) for entry in range(near)]
        spread = picked(
            hit_rows,
            [
                jnp.concatenate([back[entry][axis] for entry in range(near)], axis=0)
                for axis in range(3)
            ],
        )
        for axis in range(3):
            sent_f[turn, axis] = spread[axis][tiles:]
        copy_f(turn).start()
        field = combined(0, [local[axis] for axis in range(3)])
        field = [field[axis] + spread[axis][:tiles] for axis in range(3)]
        if turn == 0:
            ahead = [window[pl.ds(tiles * 8 + 3 + axis, tiles, stride=8), :] for axis in range(3)]
        else:
            copy_w(turn).wait_recv()
            ahead = [ahead_w[turn, axis] for axis in range(3)]
        window_vec = [jnp.concatenate([vec[axis], ahead[axis]], axis=0) for axis in range(3)]
        build(picked(hit_own, window_vec), local_far, slots)
        lax.fori_loop(0, tiles // 4, left_step, 0)
        for entry in range(near):
            more = combined(1 + entry, shifts_of(shift_left, entry))
            field = [field[axis] + more[axis] for axis in range(3)]
        copy_f(turn).wait_recv()
        return [vec[axis] * alpha_inv - (field[axis] + back_f[turn, axis]) for axis in range(3)]

    def dot_rows(left, right):
        total = left[0] * right[0] + left[1] * right[1] + left[2] * right[2]
        return jnp.sum(total, axis=0, keepdims=True)

    def send_dots(turn, resid, w):
        dots[turn, 0] = jnp.where(
            sub_ids == 0, dot_rows(resid, resid), jnp.where(sub_ids == 1, dot_rows(resid, w), 0.0)
        )

        def send(step, carry):
            pltpu.make_async_remote_copy(
                src_ref=dots.at[turn, 0],
                dst_ref=dots.at[turn, step],
                send_sem=dot_sem.at[0, turn],
                recv_sem=dot_sem.at[1, turn],
                device_id={"gx": lax.rem(me + step, count)},
                device_id_type=MESH,
            ).start()
            return carry

        lax.fori_loop(1, count, send, 0)

    def wait_dots(turn, which):
        whole = dots.at[turn, pl.ds(1, count - 1)]
        pltpu.make_async_copy(whole, whole, dot_sem.at[which, turn]).wait()

    resid = [window[pl.ds(3 + axis, tiles, stride=8), :] for axis in range(3)]
    w = applied(0, resid)
    solution = direction = s = z = None
    norm_last = step_last = None
    for turn in range(ITERS):
        more_turns = turn + 1 < ITERS
        if more_turns:
            for axis in range(3):
                sent_w[turn + 1, axis] = w[axis]
            copy_w(turn + 1).start()
        send_dots(turn, resid, w)
        if more_turns:
            q = applied(turn + 1, w)
        wait_dots(turn, 1)
        sums = jnp.sum(jnp.sum(dots[turn], axis=0), axis=1, keepdims=True)
        norm = sums[0:1, :]
        product_now = sums[1:2, :]
        if turn == 0:
            step = norm / product_now
            direction, s = resid, w
            solution = [step * direction[axis] for axis in range(3)]
            if more_turns:
                z = q
        else:
            ratio = norm / norm_last
            step = norm / (product_now - ratio * norm / step_last)
            direction = [resid[axis] + ratio * direction[axis] for axis in range(3)]
            s = [w[axis] + ratio * s[axis] for axis in range(3)]
            solution = [solution[axis] + step * direction[axis] for axis in range(3)]
            if more_turns:
                z = [q[axis] + ratio * z[axis] for axis in range(3)]
        resid = [resid[axis] - step * s[axis] for axis in range(3)]
        if more_turns:
            w = [w[axis] - step * z[axis] for axis in range(3)]
        norm_last, step_last = norm, step

    def put_final(row, value):
        out_ref[pl.ds(row, tiles, stride=8), :] = value

    for axis in range(3):
        put_final(axis, solution[axis])
        put_final(3 + axis, resid[axis])
    put_final(6, jnp.zeros((tiles, width), F32))
    put_final(7, jnp.zeros((tiles, width), F32))

    pack_copy.wait_send()
    for turn in range(ITERS):
        if turn > 0:
            copy_w(turn).wait_send()
        copy_f(turn).wait_send()
        wait_dots(turn, 0)


def on_device(positions, polar, field_ext, tile_atom, tile_list, image_shift):
    tiles, links = tile_list.shape
    atoms = tile_atom.shape[0]
    width = atoms // tiles
    near = links - 1
    count = lax.axis_size("gx")
    pairs = (2 * width, 2 * width)
    vmem = pl.BlockSpec(memory_space=pltpu.VMEM)
    smem = pl.BlockSpec(memory_space=pltpu.SMEM)
    out = jax.ShapeDtypeStruct((3, atoms), F32)
    vectors = pltpu.VMEM((ITERS, 3, tiles, width), F32)
    tiled = jax.ShapeDtypeStruct((tiles * 8, width), F32)
    window, inverse, hits, image = pl.pallas_call(
        functools.partial(tiling_kernel, tiles, links),
        out_shape=(
            tiled,
            jax.ShapeDtypeStruct((tiles, width), jnp.int32),
            jax.ShapeDtypeStruct((2 * near * tiles, width), F32),
            jax.ShapeDtypeStruct((3, near * tiles, width), F32),
        ),
        in_specs=[smem, smem, vmem, vmem, vmem, vmem],
        out_specs=(vmem, vmem, vmem, vmem),
        scratch_shapes=[pltpu.VMEM((tiles * 8, width), F32)],
    )(
        tile_list.reshape(-1),
        image_shift.reshape(-1),
        positions,
        polar.reshape(1, atoms),
        field_ext,
        tile_atom.reshape(tiles, width),
    )
    found = pl.pallas_call(
        functools.partial(kernel, count, tiles, links),
        out_shape=tiled,
        in_specs=[vmem, vmem, vmem],
        out_specs=vmem,
        scratch_shapes=[
            pltpu.VMEM((2 * tiles * 8, width), F32),
            pltpu.VMEM((tiles,) + pairs, BF16),
            pltpu.VMEM((near * tiles,) + pairs, BF16),
            pltpu.VMEM((near * tiles,) + pairs, BF16),
            pltpu.VMEM((near, width, width), F32),
            pltpu.VMEM((near, width, width), F32),
            pltpu.VMEM((near * tiles * 8, width), F32),
            pltpu.VMEM((3, tiles, width), F32),
            pltpu.VMEM((3, near * tiles, width), F32),
            pltpu.VMEM((3, near * tiles, width), F32),
            pltpu.VMEM((3, near * tiles, width), F32),
            pltpu.VMEM((near * tiles * ROWS, width), F32),
            pltpu.VMEM((near * tiles * ROWS, width), F32),
            pltpu.VMEM(((1 + near) * tiles * ROWS, width), F32),
            vectors,
            vectors,
            vectors,
            vectors,
            pltpu.VMEM((ITERS, count, 8, width), F32),
            pltpu.SemaphoreType.DMA((2,)),
            pltpu.SemaphoreType.DMA((2, ITERS)),
            pltpu.SemaphoreType.DMA((2, ITERS)),
            pltpu.SemaphoreType.DMA((2, ITERS)),
        ],
        compiler_params=pltpu.CompilerParams(collective_id=0, has_side_effects=True),
    )(window, hits, image)
    return pl.pallas_call(
        functools.partial(untiling_kernel, tiles),
        out_shape=(out, out),
        in_specs=[vmem, vmem],
        out_specs=(vmem, vmem),
    )(found, inverse)


def solution(mesh):
    in_specs = (
        P(None, ("rep", "gx")),
        P(("rep", "gx")),
        P(None, ("rep", "gx")),
        P(("rep", "gx")),
        P(("rep", "gx"), None),
        P(None, ("rep", "gx"), None),
    )
    out_specs = (P(None, ("rep", "gx")), P(None, ("rep", "gx")))
    return jax.shard_map(
        on_device, mesh=mesh, in_specs=in_specs, out_specs=out_specs, check_vma=False
    )
```

```python
import functools

import jax
import jax.numpy as jnp
from jax import lax
from jax.experimental import pallas as pl
from jax.experimental.pallas import tpu as pltpu
from jax.sharding import PartitionSpec as P

ITERS = 4
MESH = pl.DeviceIdType.MESH
thole_factor = 0.39
ROWS = 16
F32 = jnp.float32
BF16 = jnp.bfloat16


def split_two(value):
    high = value.astype(BF16)
    return high, (value - high.astype(F32)).astype(BF16)


def split_three(value):
    high = value.astype(BF16)
    rest = value - high.astype(F32)
    middle = rest.astype(BF16)
    return high, middle, (rest - middle.astype(F32)).astype(BF16)


def gather_tile(row, source, tiles):
    width = 128
    inner = jnp.broadcast_to(row & (width - 1), (8, width))
    outer = jnp.broadcast_to(row >> 7, (8, width))
    value = jnp.zeros((8, width), F32)
    for tile in range(tiles):
        picked = jnp.take_along_axis(
            source[pl.ds(tile * 8, 8), :], inner, axis=1, mode="promise_in_bounds"
        )
        value = jnp.where(outer == tile, picked, value)
    return value


def tiling_kernel(
    tiles,
    links,
    list_ref,
    shift_ref,
    place_ref,
    polar_ref,
    field_ref,
    atom_ref,
    out_ref,
    inverse,
    hits,
    image,
    feat,
):
    width = 128
    near = links - 1
    for tile in range(tiles):
        lanes = pl.ds(tile * width, width)
        feat[tile * 8 : tile * 8 + 3, :] = place_ref[:, lanes]
        feat[tile * 8 + 3 : tile * 8 + 6, :] = field_ref[:, lanes]
        feat[tile * 8 + 6 : tile * 8 + 7, :] = polar_ref[:, lanes]
        feat[tile * 8 + 7 : tile * 8 + 8, :] = jnp.ones((1, width), F32)
    sub_ids = lax.broadcasted_iota(jnp.int32, (8, width), 0)

    def fill(tile, carry):
        value = gather_tile(atom_ref[pl.ds(tile, 1), :], feat, tiles)
        root = lax.rsqrt(value)
        value = jnp.where(sub_ids == 7, pltpu.roll(root, 1, 0), value)
        out_ref[pl.ds(pl.multiple_of(tile * 8, 8), 8), :] = value
        return carry

    lax.fori_loop(0, tiles, fill, 0, unroll=4)

    lane_ids = lax.broadcasted_iota(jnp.int32, (width, width), 0)
    tile_ids = lax.broadcasted_iota(jnp.int32, (tiles, width), 0)
    lane_row = lax.broadcasted_iota(jnp.int32, (tiles, width), 1).astype(F32)

    def invert(tile, total):
        row = atom_ref[pl.ds(tile, 1), :]
        outer = tile_ids == (row >> 7)
        number = jnp.full((tiles, width), tile, jnp.int32).astype(F32)
        left = jnp.concatenate(
            [jnp.where(outer, number, 0.0), jnp.where(outer, lane_row, 0.0)], axis=0
        ).astype(BF16)
        right = jnp.where(lane_ids == (row & (width - 1)), 1.0, 0.0).astype(BF16)
        return total + lax.dot_general(
            left, right, (((1,), (1,)), ((), ())), preferred_element_type=F32
        )

    found = lax.fori_loop(
        0, tiles, invert, jnp.zeros((2 * tiles, width), F32), unroll=4
    )
    inverse[...] = (found[:tiles] * float(width) + found[tiles:]).astype(jnp.int32)

    lane_one = lax.broadcasted_iota(jnp.int32, (1, width), 1)

    def name(tile, carry):
        for entry in range(near):
            slot = entry * tiles + tile
            named = list_ref[tile * links + entry + 1]
            hit = jnp.where((lane_one == named) | (lane_one == named + 2 * tiles), 1.0, 0.0)
            hits[pl.ds(slot, 1), :] = hit
            hits[pl.ds(near * tiles + slot, 1), :] = hit
            ones = jnp.ones((1, width), F32)
            crossing = jnp.where(named >= tiles, 1.0, 0.0)
            step_y = shift_ref[tile * links + entry + 1].astype(F32)
            step_z = shift_ref[(tiles + tile) * links + entry + 1].astype(F32)
            image[0, pl.ds(slot, 1), :] = ones * crossing
            image[1, pl.ds(slot, 1), :] = ones * step_y
            image[2, pl.ds(slot, 1), :] = ones * step_z
        return carry

    lax.fori_loop(0, tiles, name, 0, unroll=4)


def untiling_kernel(tiles, tiled_ref, inverse, dip_ref, res_ref):
    width = 128

    def give(tile, carry):
        value = gather_tile(inverse[pl.ds(tile, 1), :], tiled_ref, tiles)
        lanes = pl.ds(pl.multiple_of(tile * width, width), width)
        dip_ref[:, lanes] = value[0:3]
        res_ref[:, lanes] = value[3:6]
        return carry

    lax.fori_loop(0, tiles, give, 0, unroll=4)


def kernel(
    count,
    tiles,
    links,
    tiled_ref,
    hits_ref,
    image_ref,
    out_ref,
    window,
    pair_own,
    pair_back,
    pair_left,
    three_t,
    five_t,
    there,
    local,
    local_far,
    shift_left,
    shift_right,
    moments,
    minus,
    results,
    sent_w,
    ahead_w,
    sent_f,
    back_f,
    dots,
    pack_sem,
    w_sem,
    f_sem,
    dot_sem,
):
    width = 128
    near = links - 1
    me = lax.axis_index("gx")
    after = lax.rem(me + 1, count)
    before = lax.rem(me + count - 1, count)

    barrier = pltpu.get_barrier_semaphore()

    def greet(step, carry):
        pl.semaphore_signal(
            barrier, inc=1, device_id={"gx": lax.rem(me + step, count)}, device_id_type=MESH
        )
        return carry

    lax.fori_loop(1, count, greet, 0)

    sub_ids = lax.broadcasted_iota(jnp.int32, (8, width), 0)

    window[0 : tiles * 8, :] = tiled_ref[...]
    pl.semaphore_wait(barrier, count - 1)
    pack_copy = pltpu.make_async_remote_copy(
        src_ref=tiled_ref,
        dst_ref=window.at[pl.ds(tiles * 8, tiles * 8)],
        send_sem=pack_sem.at[0],
        recv_sem=pack_sem.at[1],
        device_id={"gx": before},
        device_id_type=MESH,
    )
    pack_copy.start()

    row_ids = lax.broadcasted_iota(jnp.int32, (16, width), 0)
    column_ids = lax.broadcasted_iota(jnp.int32, (16, width), 1)

    def pair_rows(columns, other, first, same):
        rows = slice(first, first + 16)
        off_x = other[0:1, :] - columns[rows, 0:1]
        off_y = other[1:2, :] - columns[rows, 1:2]
        off_z = other[2:3, :] - columns[rows, 2:3]
        dist_sq = off_x * off_x + off_y * off_y + off_z * off_z
        if same:
            mask = row_ids + first == column_ids
            dist_sq = jnp.where(mask, 1.0, dist_sq)
        inv = lax.rsqrt(dist_sq)
        inv_sq = inv * inv
        damp = dist_sq * dist_sq * inv * (columns[rows, 7:8] * (thole_factor * other[7:8, :]))
        decay = jnp.exp(-damp)
        inv_cube = inv * inv_sq
        if same:
            inv_cube = jnp.where(mask, 0.0, inv_cube)
        less = 1.0 - decay
        three = less * inv_cube
        five = 3.0 * (less - damp * decay) * (inv_cube * inv_sq)
        return three, five

    def store_pair(target, index, first, three, five):
        rows = slice(first, first + 16)
        more = slice(width + first, width + first + 16)
        high, low = split_two(five)
        target[index, rows, 0:width] = high
        target[index, rows, width : 2 * width] = low
        high, low = split_two(three)
        target[index, more, 0:width] = high
        target[index, more, width : 2 * width] = low

    def own_pairs(tile, carry):
        here = window[pl.ds(pl.multiple_of(tile * 8, 8), 8), :]
        columns = here.T
        for first in range(0, width, 16):
            three, five = pair_rows(columns, here, first, True)
            store_pair(pair_own, tile, first, three, five)
        return carry

    lax.fori_loop(0, tiles, own_pairs, 0)

    pack_copy.wait_recv()

    slots = near * tiles
    hit_own = hits_ref[0:slots, :].astype(BF16)
    hit_rows = hits_ref[...].T[0 : 2 * tiles].astype(BF16)

    def picked(matrix, values):
        high, middle, low = split_three(jnp.concatenate(values, axis=1))
        found = jnp.dot(
            matrix, jnp.concatenate([high, middle], axis=0), preferred_element_type=F32
        ) + jnp.dot(
            matrix,
            jnp.concatenate([low, jnp.zeros_like(low)], axis=0),
            preferred_element_type=F32,
        )
        return [found[:, part * width : (part + 1) * width] for part in range(len(values))]

    def middle_of(value):
        return jnp.floor(jnp.mean(value, axis=1, keepdims=True) + 0.5)

    both = [window[pl.ds(row, 2 * tiles, stride=8), :] for row in (0, 1, 2, 7)]
    named = picked(hit_own, both)
    there[pl.ds(7, slots, stride=8), :] = named[3]
    lengths = (jnp.where(me == count - 1, 4.0 * count, 0.0), 128.0, 2.0 * tiles)
    for axis in range(3):
        here = both[axis][0:tiles]
        here_middle = middle_of(here)
        local[axis] = here - here_middle
        far_middle = middle_of(named[axis])
        local_far[axis] = named[axis] - far_middle
        vector = image_ref[axis] * lengths[axis]
        moved = named[axis] + vector
        there[pl.ds(axis, slots, stride=8), :] = moved
        for entry in range(near):
            part = slice(entry * tiles, (entry + 1) * tiles)
            shift_left[axis, part, :] = here - (far_middle[part] + vector[part])
            shift_right[axis, part, :] = moved[part] - here_middle

    def far_pairs(tile, carry):
        here_rows = pl.ds(pl.multiple_of(tile * 8, 8), 8)
        here = window[here_rows, :]
        columns = here.T
        for entry in range(near):
            slot = entry * tiles + tile
            other = there[pl.ds(pl.multiple_of(slot * 8, 8), 8), :]
            for first in range(0, width, 16):
                three, five = pair_rows(columns, other, first, False)
                store_pair(pair_back, slot, first, three, five)
                three_t[entry, first : first + 16, :] = three
                five_t[entry, first : first + 16, :] = five
            three = three_t[entry].T
            five = five_t[entry].T
            for first in range(0, width, 16):
                store_pair(
                    pair_left, slot, first, three[first : first + 16], five[first : first + 16]
                )
        return carry

    lax.fori_loop(0, tiles, far_pairs, 0)
    minus[...] = jnp.zeros_like(minus)

    def build(vec, base_ref, size):
        base = [base_ref[axis] for axis in range(3)]
        along = base[0] * vec[0] + base[1] * vec[1] + base[2] * vec[2]

        def put(ref, row, value):
            ref[pl.ds(row, size, stride=ROWS), :] = value

        for axis in range(3):
            put(moments, axis, base[axis] * along)
            put(minus, axis, -vec[axis])
            for other in range(3):
                put(moments, 4 + 4 * axis + other, base[other] * vec[axis])
            put(moments, 7 + 4 * axis, vec[axis])
        put(moments, 3, along)

    def block_of(tile):
        rows = pl.ds(pl.multiple_of(tile * ROWS, ROWS), ROWS)
        return jnp.concatenate(
            [
                jnp.concatenate(split_three(moments[rows, :]), axis=0),
                jnp.concatenate(split_three(minus[rows, :]), axis=0),
            ],
            axis=1,
        )

    def product(block, weights, slot):
        out = jnp.dot(block, weights, preferred_element_type=F32)
        out = out[:, :width] + out[:, width:]
        results[pl.ds(pl.multiple_of(slot * ROWS, ROWS), ROWS), :] = (
            out[0:ROWS] + out[ROWS : 2 * ROWS]
        ) + out[2 * ROWS : 3 * ROWS]

    def combined(kind, shifts):
        def get(row):
            return results[pl.ds(kind * tiles * ROWS + row, tiles, stride=ROWS), :]

        parts = []
        for row in range(4):
            total = get(row)
            for axis in range(3):
                total = total - shifts[axis] * get(4 + 4 * axis + row)
            parts.append(total)
        return [parts[axis] - shifts[axis] * parts[3] for axis in range(3)]

    def shifts_of(ref, entry):
        return [ref[axis, entry * tiles : (entry + 1) * tiles, :] for axis in range(3)]

    alpha_inv = 1.0 / window[pl.ds(6, tiles, stride=8), :]

    def copy_w(turn):
        return pltpu.make_async_remote_copy(
            src_ref=sent_w.at[turn],
            dst_ref=ahead_w.at[turn],
            send_sem=w_sem.at[0, turn],
            recv_sem=w_sem.at[1, turn],
            device_id={"gx": before},
            device_id_type=MESH,
        )

    def copy_f(turn):
        return pltpu.make_async_remote_copy(
            src_ref=sent_f.at[turn],
            dst_ref=back_f.at[turn],
            send_sem=f_sem.at[0, turn],
            recv_sem=f_sem.at[1, turn],
            device_id={"gx": after},
            device_id_type=MESH,
        )

    def back_step(group, carry):
        for offset in range(4):
            tile = group * 4 + offset
            block = block_of(tile)
            product(block, pair_own[tile], tile)
            for entry in range(near):
                slot = entry * tiles + tile
                product(block, pair_back[slot], tiles + slot)
        return carry

    def left_step(group, carry):
        for offset in range(4):
            tile = group * 4 + offset
            for entry in range(near):
                slot = entry * tiles + tile
                product(block_of(slot), pair_left[slot], tiles + slot)
        return carry

    def applied(turn, vec):
        build(vec, local, tiles)
        lax.fori_loop(0, tiles // 4, back_step, 0)
        back = [combined(1 + entry, shifts_of(shift_right, entry)) for entry in range(near)]
        spread = picked(
            hit_rows,
            [
                jnp.concatenate([back[entry][axis] for entry in range(near)], axis=0)
                for axis in range(3)
            ],
        )
        for axis in range(3):
            sent_f[turn, axis] = spread[axis][tiles:]
        copy_f(turn).start()
        field = combined(0, [local[axis] for axis in range(3)])
        field = [field[axis] + spread[axis][:tiles] for axis in range(3)]
        if turn == 0:
            ahead = [window[pl.ds(tiles * 8 + 3 + axis, tiles, stride=8), :] for axis in range(3)]
        else:
            copy_w(turn).wait_recv()
            ahead = [ahead_w[turn, axis] for axis in range(3)]
        window_vec = [jnp.concatenate([vec[axis], ahead[axis]], axis=0) for axis in range(3)]
        build(picked(hit_own, window_vec), local_far, slots)
        lax.fori_loop(0, tiles // 4, left_step, 0)
        for entry in range(near):
            more = combined(1 + entry, shifts_of(shift_left, entry))
            field = [field[axis] + more[axis] for axis in range(3)]
        copy_f(turn).wait_recv()
        return [vec[axis] * alpha_inv - (field[axis] + back_f[turn, axis]) for axis in range(3)]

    def dot_rows(left, right):
        total = left[0] * right[0] + left[1] * right[1] + left[2] * right[2]
        return jnp.sum(total, axis=0, keepdims=True)

    def send_dots(turn, resid, w):
        dots[turn, 0] = jnp.where(
            sub_ids == 0, dot_rows(resid, resid), jnp.where(sub_ids == 1, dot_rows(resid, w), 0.0)
        )

        def send(step, carry):
            pltpu.make_async_remote_copy(
                src_ref=dots.at[turn, 0],
                dst_ref=dots.at[turn, step],
                send_sem=dot_sem.at[0, turn],
                recv_sem=dot_sem.at[1, turn],
                device_id={"gx": lax.rem(me + step, count)},
                device_id_type=MESH,
            ).start()
            return carry

        lax.fori_loop(1, count, send, 0)

    def wait_dots(turn, which):
        whole = dots.at[turn, pl.ds(1, count - 1)]
        pltpu.make_async_copy(whole, whole, dot_sem.at[which, turn]).wait()

    resid = [window[pl.ds(3 + axis, tiles, stride=8), :] for axis in range(3)]
    w = applied(0, resid)
    solution = direction = s = z = None
    norm_last = step_last = None
    for turn in range(ITERS):
        more_turns = turn + 1 < ITERS
        if more_turns:
            for axis in range(3):
                sent_w[turn + 1, axis] = w[axis]
            copy_w(turn + 1).start()
        send_dots(turn, resid, w)
        if more_turns:
            q = applied(turn + 1, w)
        wait_dots(turn, 1)
        sums = jnp.sum(jnp.sum(dots[turn], axis=0), axis=1, keepdims=True)
        norm = sums[0:1, :]
        product_now = sums[1:2, :]
        if turn == 0:
            step = norm / product_now
            direction, s = resid, w
            solution = [step * direction[axis] for axis in range(3)]
            if more_turns:
                z = q
        else:
            ratio = norm / norm_last
            step = norm / (product_now - ratio * norm / step_last)
            direction = [resid[axis] + ratio * direction[axis] for axis in range(3)]
            s = [w[axis] + ratio * s[axis] for axis in range(3)]
            solution = [solution[axis] + step * direction[axis] for axis in range(3)]
            if more_turns:
                z = [q[axis] + ratio * z[axis] for axis in range(3)]
        resid = [resid[axis] - step * s[axis] for axis in range(3)]
        if more_turns:
            w = [w[axis] - step * z[axis] for axis in range(3)]
        norm_last, step_last = norm, step

    def put_final(row, value):
        out_ref[pl.ds(row, tiles, stride=8), :] = value

    for axis in range(3):
        put_final(axis, solution[axis])
        put_final(3 + axis, resid[axis])
    put_final(6, jnp.zeros((tiles, width), F32))
    put_final(7, jnp.zeros((tiles, width), F32))

    pack_copy.wait_send()
    for turn in range(ITERS):
        if turn > 0:
            copy_w(turn).wait_send()
        copy_f(turn).wait_send()
        wait_dots(turn, 0)


def on_device(positions, polar, field_ext, tile_atom, tile_list, image_shift):
    tiles, links = tile_list.shape
    atoms = tile_atom.shape[0]
    width = atoms // tiles
    near = links - 1
    count = lax.axis_size("gx")
    pairs = (2 * width, 2 * width)
    vmem = pl.BlockSpec(memory_space=pltpu.VMEM)
    smem = pl.BlockSpec(memory_space=pltpu.SMEM)
    out = jax.ShapeDtypeStruct((3, atoms), F32)
    vectors = pltpu.VMEM((ITERS, 3, tiles, width), F32)
    tiled = jax.ShapeDtypeStruct((tiles * 8, width), F32)
    window, inverse, hits, image = pl.pallas_call(
        functools.partial(tiling_kernel, tiles, links),
        out_shape=(
            tiled,
            jax.ShapeDtypeStruct((tiles, width), jnp.int32),
            jax.ShapeDtypeStruct((2 * near * tiles, width), F32),
            jax.ShapeDtypeStruct((3, near * tiles, width), F32),
        ),
        in_specs=[smem, smem, vmem, vmem, vmem, vmem],
        out_specs=(vmem, vmem, vmem, vmem),
        scratch_shapes=[pltpu.VMEM((tiles * 8, width), F32)],
    )(
        tile_list.reshape(-1),
        image_shift.reshape(-1),
        positions,
        polar.reshape(1, atoms),
        field_ext,
        tile_atom.reshape(tiles, width),
    )
    found = pl.pallas_call(
        functools.partial(kernel, count, tiles, links),
        out_shape=tiled,
        in_specs=[vmem, vmem, vmem],
        out_specs=vmem,
        scratch_shapes=[
            pltpu.VMEM((2 * tiles * 8, width), F32),
            pltpu.VMEM((tiles,) + pairs, BF16),
            pltpu.VMEM((near * tiles,) + pairs, BF16),
            pltpu.VMEM((near * tiles,) + pairs, BF16),
            pltpu.VMEM((near, width, width), F32),
            pltpu.VMEM((near, width, width), F32),
            pltpu.VMEM((near * tiles * 8, width), F32),
            pltpu.VMEM((3, tiles, width), F32),
            pltpu.VMEM((3, near * tiles, width), F32),
            pltpu.VMEM((3, near * tiles, width), F32),
            pltpu.VMEM((3, near * tiles, width), F32),
            pltpu.VMEM((near * tiles * ROWS, width), F32),
            pltpu.VMEM((near * tiles * ROWS, width), F32),
            pltpu.VMEM(((1 + near) * tiles * ROWS, width), F32),
            vectors,
            vectors,
            vectors,
            vectors,
            pltpu.VMEM((ITERS, count, 8, width), F32),
            pltpu.SemaphoreType.DMA((2,)),
            pltpu.SemaphoreType.DMA((2, ITERS)),
            pltpu.SemaphoreType.DMA((2, ITERS)),
            pltpu.SemaphoreType.DMA((2, ITERS)),
        ],
        compiler_params=pltpu.CompilerParams(collective_id=0, has_side_effects=True),
    )(window, hits, image)
    return pl.pallas_call(
        functools.partial(untiling_kernel, tiles),
        out_shape=(out, out),
        in_specs=[vmem, vmem],
        out_specs=(vmem, vmem),
    )(found, inverse)


def solution(mesh):
    in_specs = (
        P(None, ("rep", "gx")),
        P(("rep", "gx")),
        P(None, ("rep", "gx")),
        P(("rep", "gx")),
        P(("rep", "gx"), None),
        P(None, ("rep", "gx"), None),
    )
    out_specs = (P(None, ("rep", "gx")), P(None, ("rep", "gx")))
    return jax.shard_map(
        on_device, mesh=mesh, in_specs=in_specs, out_specs=out_specs, check_vma=False
    )
```
